32 devices in a mesh: replica: 8 (over z, core), ctx: 4 (over y, x).
Axes of the slice: x: 2, y: 2, z: 4, core: 2. Of those that a mesh axis runs over, the one named last changes fastest.
Arguments:
- queries: bfloat16 [32, 128, 3584], P('replica', 'ctx'), may hold values from -128 to 128
- key_cache: bfloat16 [4096, 512], P('ctx'), may hold values from -6 to 6
- value_cache: bfloat16 [4096, 512], P('ctx'), may hold values from -6 to 6
- key_scale: float32 [32, 4], P('ctx'), may hold values from 0.7 to 1.4
- value_scale: float32 [32, 4], P('ctx'), may hold values from 0.5 to 2
- pattern: int32 [28, 32, 32], replicated, may hold values from 0 to 31
- target: int32 [32], replicated, may hold values from 0 to 7, as said below
Outputs:
- landed: bfloat16 [32, 128, 3584], P('replica', 'ctx')
The draws below stay inside these ranges and needn't reach their ends.
Inputs may be any that keep to these rules, and one draw needn't show every extreme that they name: `target`: query block j belongs to group j // 4. The blocks of one group go to distinct groups, and every group receives exactly 4 blocks.
All inputs are finite; a program needn't handle non-finite values.
Results may differ from the reference program's by a relative error of at most 0.018.
Values may be sent and summed in bfloat16 or wider, within the bound.
No kernel may reach another device: no remote copies, remote signals or barrier semaphores. Data moves between devices by JAX's collectives and lax.ppermute only.
A program may use at most 64 MiB of HBM per device.

```python
import math
import jax
import jax.numpy as jnp
from jax import lax

HEADS = 28
KV_HEADS = 4
HEAD_DIM = 128
BLOCK = 128
SELECTED = 32
CTX_DEV = 1024
QBLK_DEV = 4
GROUPS = 8
SHARDS = 4
QBLOCKS = 32
KVBLOCKS = 32


def paired_draw(key):
    folded = jax.random.fold_in(key, 5)
    query_key, cache_key = jax.random.split(folded, 2)
    row_width = HEADS * HEAD_DIM
    query_base = jax.random.truncated_normal(query_key, -6.0, 6.0, (QBLOCKS, BLOCK, row_width), jnp.float32)
    cache_base = jax.random.truncated_normal(cache_key, -6.0, 6.0, (KVBLOCKS * BLOCK, KV_HEADS * HEAD_DIM), jnp.float32)
    return (query_base, cache_base)


def draw_queries(key, part):
    return paired_draw(key)[0].astype(jnp.bfloat16)


def draw_key_cache(key, part):
    return paired_draw(key)[1].astype(jnp.bfloat16)


def draw_target(key, part):
    first_key, second_key = jax.random.split(jax.random.fold_in(key, 11))
    ordering = jax.random.permutation(first_key, GROUPS)
    shifts = jax.random.permutation(second_key, GROUPS)[:QBLK_DEV]
    inverse = jnp.argsort(ordering)
    return ordering[(inverse[:, None] + shifts[None, :]) % GROUPS].reshape(QBLOCKS).astype(jnp.int32)


def set_ends(array, own_key, smallest, top_value):
    extent = array.shape
    index_at = [jax.random.randint(jax.random.fold_in(own_key, axis), (), 0, extent[axis]) for axis in range(len(extent))]
    array = array.at[tuple(index_at)].set(smallest)
    longest = extent.index(max(extent))
    index_at[longest] = (index_at[longest] + 1) % extent[longest]
    return array.at[tuple(index_at)].set(top_value)


def block_scale(rng, dims, pieces, least, top_value):
    level, own = 1.0, jax.random.fold_in(rng, 6)
    for position, parts in pieces:
        draws = jnp.exp(jax.random.uniform(jax.random.fold_in(own, position), (parts,), jnp.float32, least / len(pieces), top_value / len(pieces)))
        level = level * jnp.repeat(draws, dims[position] // parts).reshape([-1 if axis == position else 1 for axis in range(len(dims))])
    return level


def bell_draw(own_key, extent, scale, limit, cuts=(), kind=jnp.bfloat16):
    result = jax.random.normal(own_key, extent, jnp.float32) * scale
    if len(cuts) > 0:
        result = block_scale(own_key, extent, cuts, -0.22, 0.18) * result
    return jnp.clip(result, min=-limit, max=limit).astype(kind)


def setup_inputs(seed: int = 0) -> dict:
    splits = jax.random.split(jax.random.key(seed), 8)
    queries = draw_queries(jax.random.fold_in(splits[7], 71), 0)
    key_cache = draw_key_cache(jax.random.fold_in(splits[7], 71), 0)
    value_cache = bell_draw(splits[2], (KVBLOCKS * BLOCK, KV_HEADS * HEAD_DIM), 1.0, 6.0, ((0, 4),))
    key_scale = jnp.clip(jnp.exp(math.log(1.4) - 0.6931472 * jax.random.uniform(splits[3], (KVBLOCKS, KV_HEADS), jnp.float32) ** block_scale(splits[3], (KVBLOCKS, KV_HEADS), ((0, 4),), -0.2, 0.2)), 0.7, 1.4)
    value_scale = jnp.clip(jnp.exp(math.log(2.0) - 1.3862944 * jax.random.uniform(splits[4], (KVBLOCKS, KV_HEADS), jnp.float32) ** block_scale(splits[4], (KVBLOCKS, KV_HEADS), ((0, 4),), -0.2, 0.2)), 0.5, 2.0)
    pattern = set_ends(jax.random.randint(splits[5], (HEADS, QBLOCKS, SELECTED), 0, KVBLOCKS), jax.random.fold_in(splits[5], 1), 0, KVBLOCKS - 1).astype(jnp.int32)
    target = draw_target(jax.random.fold_in(splits[7], 71), 0)
    return dict(queries=queries, key_cache=key_cache, value_cache=value_cache, key_scale=key_scale, value_scale=value_scale, pattern=pattern, target=target)


def reference(queries, key_cache, value_cache, key_scale, value_scale, pattern, target):
    group_size = HEADS // KV_HEADS
    local_blocks = CTX_DEV // BLOCK
    first_block = KVBLOCKS - QBLOCKS
    inv_root = 1.0 / math.sqrt(HEAD_DIM)
    keys_all = key_cache.astype(jnp.float32).reshape(SHARDS, local_blocks, BLOCK, KV_HEADS, HEAD_DIM)
    values_all = value_cache.astype(jnp.float32).reshape(SHARDS, local_blocks, BLOCK, KV_HEADS, HEAD_DIM)
    key_factor = jnp.transpose(key_scale.reshape(SHARDS, local_blocks, KV_HEADS), (2, 0, 1)) * inv_root
    value_factor = jnp.transpose(value_scale.reshape(SHARDS, local_blocks, KV_HEADS), (2, 0, 1))
    block_ids = jnp.arange(KVBLOCKS, dtype=jnp.int32)
    key_pos = jnp.arange(KVBLOCKS * BLOCK, dtype=jnp.int32).reshape(SHARDS, local_blocks, BLOCK)
    row_ids = jnp.arange(BLOCK, dtype=jnp.int32)

    def one_block(operands):
        query_block, listed, block_index = operands
        diagonal = first_block + block_index
        chosen = jnp.any(listed[:, :, None] == block_ids[None, None, :], axis=1) | (block_ids == diagonal)[None, :]
        chosen = chosen.reshape(KV_HEADS, group_size, SHARDS, local_blocks)
        query_pos = diagonal * BLOCK + row_ids
        causal = key_pos[None] <= query_pos[:, None, None, None]
        allowed = chosen[:, :, None, :, :, None] & causal[None, None]
        query_f = query_block.astype(jnp.float32).reshape(BLOCK, KV_HEADS, group_size, HEAD_DIM)
        scores = jnp.einsum('rgkd,sbtgd->gkrsbt', query_f, keys_all) * key_factor[:, None, None, :, :, None]
        local_top = lax.optimization_barrier(jnp.max(jnp.where(allowed, scores, -jnp.inf), axis=(4, 5), keepdims=True))
        top_score = lax.optimization_barrier(jnp.max(local_top, axis=3, keepdims=True))
        rescale = jnp.exp(local_top - top_score)
        expo = jnp.where(allowed, jnp.exp(scores - local_top), 0.0)
        weight = (expo * value_factor[:, None, None, :, :, None]).astype(jnp.bfloat16)
        weight = lax.optimization_barrier(weight).astype(jnp.float32)
        rescale_t = jnp.transpose(rescale[:, :, :, :, 0, 0], (3, 2, 0, 1))
        numer_part = (jnp.einsum('gkrsbt,sbtgd->srgkd', weight, values_all) * rescale_t[..., None]).astype(jnp.bfloat16)
        denom_part = (jnp.transpose(lax.optimization_barrier(jnp.sum(expo, axis=(4, 5))), (3, 2, 0, 1)) * rescale_t).astype(jnp.bfloat16)
        numer_part = lax.optimization_barrier(numer_part)
        denom_part = lax.optimization_barrier(denom_part)
        numer_sum = lax.optimization_barrier(jnp.sum(numer_part.astype(jnp.float32), axis=0))
        denom_sum = lax.optimization_barrier(jnp.sum(denom_part.astype(jnp.float32), axis=0))
        attended = numer_sum / denom_sum[..., None]
        return attended.reshape(BLOCK, HEADS * HEAD_DIM).astype(jnp.bfloat16)
    attended_all = lax.map(one_block, (queries, jnp.transpose(pattern, (1, 0, 2)), jnp.arange(QBLOCKS, dtype=jnp.int32)))
    arrival_order = jnp.argsort(target, stable=True).astype(jnp.int32)
    return jnp.take(attended_all, arrival_order, axis=0)
```

```python
import functools
import math

import jax
import jax.numpy as jnp
from jax import lax
from jax.experimental import pallas as pl
from jax.experimental.pallas import tpu as pltpu
from jax.sharding import PartitionSpec as P


MASKED = -1e30
NT = (((1,), (1,)), ((), ()))


def routes(target, group_count, per_group):
    grid = target.reshape(group_count, per_group)
    groups = jnp.arange(group_count, dtype=jnp.int32)
    hit = (grid[:, :, None] == groups[None, None, :]).astype(jnp.int32)
    slot = jnp.sum(hit * jnp.arange(per_group, dtype=jnp.int32)[None, :, None], axis=1)
    coming = jnp.sum(hit, axis=1)
    return coming, slot


def attend_kernel(
    row_count,
    heads,
    diag_ref,
    source_ref,
    scale_ref,
    q_ref,
    k_ref,
    v_ref,
    bias_ref,
    out_ref,
    q_aug,
    k_aug,
    v_aug,
    score,
    top,
    acc,
):
    slot = pl.program_id(0)
    part = pl.program_id(1)
    rows = row_count
    width = k_ref.shape[2]
    kv_blocks = bias_ref.shape[1]
    group = bias_ref.shape[2]
    chunks = q_ref.shape[1]

    @pl.when((slot == 0) & (part == 0))
    def _():
        for i in range(k_ref.shape[0]):
            span = k_ref.shape[1]
            k_aug[pl.ds(i * span, span), pl.ds(0, width)] = k_ref[i]
            v_aug[pl.ds(i * span, span), pl.ds(0, width)] = v_ref[i]
        v_aug[:, pl.ds(width, width)] = jnp.ones((v_aug.shape[0], width), jnp.bfloat16)

    @pl.when(part == 0)
    def _():
        for b in range(kv_blocks):
            k_aug[pl.ds(b * rows, rows), pl.ds(width, width)] = jnp.broadcast_to(
                bias_ref[0, pl.ds(b, 1), :], (rows, group)
            ).astype(jnp.bfloat16)

    lane = lax.broadcasted_iota(jnp.int32, (rows, width), 1)
    for r in range(heads):
        piece = q_ref[0, :, :, pl.ds(r * width, width)]
        if piece.shape[1] % 16:
            piece = piece.astype(jnp.float32)
        q_aug[pl.ds(r * rows, rows), pl.ds(0, width)] = piece.reshape(rows, width).astype(
            jnp.bfloat16
        )
        q_aug[pl.ds(r * rows, rows), pl.ds(width, width)] = (lane == part * heads + r).astype(
            jnp.bfloat16
        )

    diag = diag_ref[slot]
    pairs = (diag + 1) // 2
    end = pl.multiple_of(diag * rows, rows)
    own_scale = scale_ref[diag]
    own_key = k_aug[pl.ds(end, rows), pl.ds(0, width)]
    causal = lane <= lax.broadcasted_iota(jnp.int32, (rows, width), 0)
    hold = score.shape[1] - width
    for r in range(heads):
        span = pl.ds(r * rows, rows)
        s = lax.dot_general(
            q_aug[span, pl.ds(0, width)], own_key, NT, preferred_element_type=jnp.float32
        )
        s = jnp.where(causal, s * own_scale, MASKED)
        score[span, pl.ds(hold, width)] = s
        top[span, :] = s

    def find(i, carry):
        at = pl.multiple_of(i * 2 * rows, 2 * rows)
        key = k_aug[pl.ds(at, 2 * rows), :]
        lo = scale_ref[2 * i]
        hi = scale_ref[2 * i + 1]
        for r in range(heads):
            span = pl.ds(r * rows, rows)
            s = lax.dot_general(q_aug[span, :], key, NT, preferred_element_type=jnp.float32)
            a = s[:, :width] * lo
            b = s[:, width:] * hi
            score[span, pl.ds(at, width)] = a
            score[span, pl.ds(pl.multiple_of(at + rows, rows), width)] = b
            top[span, :] = jnp.maximum(top[span, :], jnp.maximum(a, b))
        return carry

    lax.fori_loop(0, pairs, find, 0)

    own_value = v_aug[pl.ds(end, rows), :]
    for r in range(heads):
        span = pl.ds(r * rows, rows)
        m = jnp.broadcast_to(jnp.max(top[span, :], axis=1, keepdims=True), (rows, width))
        top[span, :] = m
        p = jnp.exp2(score[span, pl.ds(hold, width)] - m).astype(jnp.bfloat16)
        acc[span, :] = jnp.dot(p, own_value, preferred_element_type=jnp.float32)

    def gather(i, carry):
        at = pl.multiple_of(i * 2 * rows, 2 * rows)
        value = v_aug[pl.ds(at, 2 * rows), :]
        for r in range(heads):
            span = pl.ds(r * rows, rows)
            m = top[span, :]
            p = jnp.exp2(
                score[span, pl.ds(at, 2 * width)] - jnp.concatenate([m, m], axis=1)
            ).astype(jnp.bfloat16)
            acc[span, :] += jnp.dot(p, value, preferred_element_type=jnp.float32)
        return carry

    lax.fori_loop(0, pairs, gather, 0)

    for r in range(heads):
        span = pl.ds(r * rows, rows)
        res = acc[span, pl.ds(0, width)] / acc[span, pl.ds(width, width)]
        if rows // chunks % 16 == 0:
            res = res.astype(jnp.bfloat16)
        out_ref[:, 0, :, pl.ds(r * width, width)] = res.reshape(
            chunks, rows // chunks, width
        ).astype(jnp.bfloat16)


def attend(received, source, diag, scale, keys, values, bias, heads_total):
    slots = source.shape[0]
    chunks, chunk_rows = received.shape[1], received.shape[2]
    rows = chunks * chunk_rows
    width = keys.shape[2]
    kv_rows = keys.shape[0] * keys.shape[1]
    kv_blocks = kv_rows // rows
    heads = heads_total
    while heads > 1 and (
        heads_total % heads or heads * rows * (kv_rows + width) * 4 > 18 * 2**20
    ):
        heads -= 1
    kernel = functools.partial(attend_kernel, rows, heads)
    once = lambda *shape: pl.BlockSpec(shape, lambda s, p, *_: (0,) * len(shape))
    grid_spec = pltpu.PrefetchScalarGridSpec(
        num_scalar_prefetch=3,
        grid=(slots, heads_total // heads),
        in_specs=[
            pl.BlockSpec(
                (1, chunks, chunk_rows, heads * width), lambda s, p, d, src, sc: (src[s], 0, 0, p)
            ),
            once(*keys.shape),
            once(*values.shape),
            pl.BlockSpec((1, kv_blocks, bias.shape[2]), lambda s, p, *_: (s, 0, 0)),
        ],
        out_specs=pl.BlockSpec(
            (chunks, 1, chunk_rows, heads * width), lambda s, p, *_: (0, s, 0, p)
        ),
        scratch_shapes=[
            pltpu.VMEM((heads * rows, 2 * width), jnp.bfloat16),
            pltpu.VMEM((kv_rows, 2 * width), jnp.bfloat16),
            pltpu.VMEM((kv_rows, 2 * width), jnp.bfloat16),
            pltpu.VMEM((heads * rows, kv_rows + width), jnp.float32),
            pltpu.VMEM((heads * rows, width), jnp.float32),
            pltpu.VMEM((heads * rows, 2 * width), jnp.float32),
        ],
    )
    work = slots * heads_total * rows * kv_rows * width
    return pl.pallas_call(
        kernel,
        grid_spec=grid_spec,
        out_shape=jax.ShapeDtypeStruct(
            (chunks, slots, chunk_rows, heads_total * width), jnp.bfloat16
        ),
        compiler_params=pltpu.CompilerParams(
            dimension_semantics=("arbitrary", "arbitrary"), vmem_limit_bytes=56 * 2**20
        ),
        cost_estimate=pl.CostEstimate(
            flops=2 * work, bytes_accessed=8 * 2**20, transcendentals=work // width // 2
        ),
        name="attend",
    )(diag, source, scale, received, keys, values, bias)


def exchange(pieces, axis, count):
    me = lax.axis_index(axis)
    own = lax.dynamic_index_in_dim(pieces, me, 0, keepdims=False)
    if count & (count - 1):
        return lax.all_to_all(pieces, axis, split_axis=0, concat_axis=0, tiled=True)
    got = [own]
    for step in range(1, count):
        piece = lax.dynamic_index_in_dim(pieces, me ^ step, 0, keepdims=False)
        got.append(lax.ppermute(piece, axis, [(i, i ^ step) for i in range(count)]))
    return got


def per_device(queries, key_cache, value_cache, key_scale, value_scale, pattern, target):
    group_count = lax.axis_size("replica")
    shard_count = lax.axis_size("ctx")
    group_index = lax.axis_index("replica")
    shard_index = lax.axis_index("ctx")
    per_group, chunk_rows, row_width = queries.shape
    rows = chunk_rows * shard_count
    kv_heads = key_scale.shape[1]
    width = key_cache.shape[1] // kv_heads
    head_count = row_width // width
    group = head_count // kv_heads
    span = group * width
    local_blocks = key_scale.shape[0]
    kv_blocks = local_blocks * shard_count
    first_block = kv_blocks - pattern.shape[1]
    repeat = shard_count // kv_heads
    slots = per_group // repeat
    my_head = shard_index // repeat
    my_part = shard_index % repeat

    coming, slot_of = routes(target, group_count, per_group)

    keys = key_cache.reshape(-1, kv_heads, width).transpose(1, 0, 2)
    scaled = (
        value_cache.astype(jnp.float32).reshape(local_blocks, rows, kv_heads, width)
        * value_scale[:, None, :, None]
    ).astype(jnp.bfloat16)
    scaled = scaled.reshape(-1, kv_heads, width).transpose(1, 0, 2)
    kv = jnp.repeat(jnp.concatenate([keys, scaled], axis=1), repeat, axis=0)
    got = lax.all_to_all(kv, "ctx", split_axis=0, concat_axis=0, tiled=True)
    kv_rows = keys.shape[1]
    all_scale = lax.all_gather(key_scale, "ctx", axis=0, tiled=True)
    scale = lax.dynamic_index_in_dim(all_scale, my_head, 1, keepdims=False) * (
        1.0 / (math.sqrt(width) * math.log(2.0))
    )

    by_head = queries.reshape(per_group, chunk_rows, kv_heads, span).transpose(0, 2, 1, 3)
    outgoing = jnp.take(by_head, slot_of[group_index], axis=0)
    outgoing = jnp.repeat(outgoing, repeat, axis=1).reshape(
        group_count * shard_count, chunk_rows, span
    )
    received = lax.all_to_all(
        outgoing, ("replica", "ctx"), split_axis=0, concat_axis=0, tiled=True
    ).reshape(group_count, shard_count, chunk_rows, span)

    mine = lax.dynamic_index_in_dim(coming, group_index, 1, keepdims=False)
    order = jnp.cumsum(mine) - 1
    places = my_part * slots + jnp.arange(slots, dtype=jnp.int32)
    match = (mine[None, :] > 0) & (order[None, :] == places[:, None])
    sources = jnp.arange(group_count, dtype=jnp.int32)
    source = jnp.sum(jnp.where(match, sources[None, :], 0), axis=1)
    block = source * per_group + jnp.sum(
        jnp.where(match, slot_of[:, group_index][None, :], 0), axis=1
    )
    diag = first_block + block

    listed = lax.dynamic_slice_in_dim(jnp.take(pattern, block, axis=1), my_head * group, group, 0)
    ids = jnp.arange(kv_blocks, dtype=jnp.int32)
    chosen = jnp.any(listed[:, :, :, None] == ids, axis=2) & (ids[None, :] < diag[:, None])[None]
    bias = jnp.where(chosen, 0.0, MASKED).transpose(1, 2, 0)
    bias = jnp.pad(bias, ((0, 0), (0, 0), (0, width - group)))

    attended = attend(
        received, source, diag, scale, got[:, :kv_rows], got[:, kv_rows:], bias, group
    )
    back = lax.all_to_all(attended, "ctx", split_axis=0, concat_axis=0, tiled=True)
    back = back.reshape(kv_heads, repeat, slots, chunk_rows, span)
    return back.transpose(1, 2, 3, 0, 4).reshape(per_group, chunk_rows, row_width)


def solution(mesh):
    return jax.shard_map(
        per_device,
        mesh=mesh,
        in_specs=(
            P("replica", "ctx", None),
            P("ctx", None),
            P("ctx", None),
            P("ctx", None),
            P("ctx", None),
            P(),
            P(),
        ),
        out_specs=P("replica", "ctx", None),
        check_vma=False,
    )
```

```python
import functools
import math

import jax
import jax.numpy as jnp
from jax import lax
from jax.experimental import pallas as pl
from jax.experimental.pallas import tpu as pltpu
from jax.sharding import PartitionSpec as P


MASKED = -1e30
SIZES = (8, 4, 2)
NT = (((1,), (1,)), ((), ()))
VMEM = pl.BlockSpec(memory_space=pltpu.VMEM)
SMEM = pl.BlockSpec(memory_space=pltpu.SMEM)


class Plan:
    def __init__(self, queries, key_cache, key_scale, pattern, groups, shards):
        self.groups, self.shards = groups, shards
        self.per_group, self.chunk, self.row_width = queries.shape
        self.rows = self.chunk * shards
        self.kv_heads = key_scale.shape[1]
        self.width = key_cache.shape[1] // self.kv_heads
        self.group = self.row_width // self.width // self.kv_heads
        self.span = self.group * self.width
        self.local_blocks = key_scale.shape[0]
        self.local_rows = key_cache.shape[0]
        self.kv_blocks = self.local_blocks * shards
        self.kv_rows = self.local_rows * shards
        self.first_block = self.kv_blocks - pattern.shape[1]
        self.repeat = shards // self.kv_heads
        self.slots = self.per_group // self.repeat
        self.scale_rows = -(-3 * self.local_blocks // 16) * 16
        self.sourced = self.group * 3 // 7
        self.landed = self.group - self.sourced
        self.stride = max(self.chunk, 16)
        self.near_rows = self.sourced * self.slots * self.stride

    def cache_rows(self, relative):
        count = 2 * self.local_rows if relative == 0 else self.local_rows
        return count + self.scale_rows


def aligned(index, size):
    return pl.ds(pl.multiple_of(index * size, size), size)


def pack_far(plan, target, q_ref, far):
    group = lax.axis_index("replica")
    wide = plan.sourced * plan.width
    for d in range(plan.shards):
        head = d // plan.repeat
        for k in range(plan.per_group):
            far[target[group * plan.per_group + k], d] = q_ref[
                k, :, pl.ds(head * plan.span + wide, plan.landed * plan.width)
            ]


def pack_near(plan, ks_ref, vs_ref, k_ref, v_ref, q_ref, *refs):
    outs, factors = refs[: plan.shards], refs[plan.shards]
    group, me = lax.axis_index("replica"), lax.axis_index("ctx")
    rows, width, blocks = plan.rows, plan.width, plan.local_blocks
    half = group % 2
    lane = lax.broadcasted_iota(jnp.int32, ks_ref.shape, 1)
    for c in range(plan.shards):
        at = me ^ c
        head, part = at // plan.repeat, at % plan.repeat
        lanes = aligned(head, width)

        def column(ref):
            picked = jnp.sum(jnp.where(lane == head, ref[...], 0.0), axis=1, keepdims=True)
            return jnp.broadcast_to(picked, (blocks, width))

        factors[...] = column(vs_ref)
        count = blocks if c == 0 else blocks // 2
        first = 0 if c == 0 else half * count
        out = outs[c]
        for i in range(count):
            b = first + i
            out[pl.ds(i * rows, rows), :] = k_ref[aligned(b, rows), lanes]
            out[pl.ds((count + i) * rows, rows), :] = (
                v_ref[aligned(b, rows), lanes].astype(jnp.float32) * factors[pl.ds(b, 1), :]
            ).astype(jnp.bfloat16)
        x = column(ks_ref)
        high = x.astype(jnp.bfloat16).astype(jnp.float32)
        middle = (x - high).astype(jnp.bfloat16).astype(jnp.float32)
        low = x - high - middle
        spare = plan.scale_rows - 3 * blocks
        terms = [high, middle, low]
        if spare:
            terms.append(jnp.zeros((spare, width), jnp.float32))
        out[pl.ds(2 * count * rows, plan.scale_rows), :] = jnp.concatenate(terms, axis=0).astype(
            jnp.bfloat16
        )
        base = plan.cache_rows(c)
        for r in range(plan.sourced):
            for k in range(plan.slots):
                out[pl.ds(base + (r * plan.slots + k) * plan.stride, plan.chunk), :] = q_ref[
                    part * plan.slots + k,
                    :,
                    pl.ds(pl.multiple_of(head * plan.span + r * width, width), width),
                ]


def attend_body(plan, far, step, *refs):
    n = plan.shards
    target, refs = refs[0], refs[1:]
    if far:
        received, keys, values, scale, pattern = refs[:5]
        outs, refs = refs[5 : 5 + n], refs[5 + n :]
    else:
        own, direct, swapped = refs[0], refs[1:n], refs[n : 2 * n - 1]
        pattern, out, keys, values, scale = refs[2 * n - 1 : 2 * n + 4]
        refs = refs[2 * n + 4 :]
    q_aug, bias_rows, score, top, acc, loose, blocks = refs

    group, me = lax.axis_index("replica"), lax.axis_index("ctx")
    rows, width, slots = plan.rows, plan.width, plan.slots
    head_count = plan.landed if far else plan.sourced
    head_first = plan.sourced if far else 0
    my_head, my_part = me // plan.repeat, me % plan.repeat
    half = group % 2

    def take(ref, count, block):
        size = count * rows
        at = pl.ds(pl.multiple_of(block * rows, rows), size)
        keys[at, :] = ref[pl.ds(0, size), :]
        values[at, :] = ref[pl.ds(size, size), :]

    if not far:
        size = plan.local_blocks
        some = size // 2
        factor = 1.0 / (math.sqrt(width) * math.log(2.0))
        for c in range(n):
            shard = me ^ c
            if c == 0:
                take(own, size, shard * size)
            else:
                take(direct[c - 1], some, shard * size + half * some)
                take(swapped[c - 1], some, shard * size + (1 - half) * some)
            tail = (own if c == 0 else direct[c - 1])[
                pl.ds(plan.cache_rows(c) - plan.scale_rows, plan.scale_rows), :
            ].astype(jnp.float32)
            scale[aligned(shard, size), :] = (
                tail[:size] + tail[size : 2 * size] + tail[2 * size : 3 * size]
            ) * factor

    if far:

        def scan(j, found):
            hit = target[j] == group

            @pl.when(hit)
            def _():
                blocks[found] = j

            return found + hit.astype(jnp.int32)

        lax.fori_loop(0, target.shape[0], scan, 0)

    lane = lax.broadcasted_iota(jnp.int32, (rows, width), 1)
    causal = lane <= lax.broadcasted_iota(jnp.int32, (rows, width), 0)
    for r in range(step):
        q_aug[pl.ds(r * rows, rows), pl.ds(width, width)] = (lane == r).astype(jnp.bfloat16)
    kv_lane = lax.broadcasted_iota(jnp.int32, (plan.kv_blocks, width), 1)
    selected = pattern.shape[2]
    kv_id = lax.broadcasted_iota(jnp.int32, (plan.kv_blocks, selected), 0)
    kv_row = lax.broadcasted_iota(jnp.int32, (plan.kv_blocks, width), 0)
    hold = score.shape[1] - width

    def one(k, head_from):
        block = blocks[my_part * slots + k] if far else (
            group * plan.per_group + my_part * slots + k
        )
        diag = plan.first_block + block
        bias = jnp.full((plan.kv_blocks, width), MASKED, jnp.float32)
        for r in range(step):
            listed = pattern[
                my_head * plan.group + head_first + head_from + r, pl.ds(block, 1), :
            ]
            hit = jnp.max(
                jnp.where(kv_id == listed, 1.0, 0.0), axis=1, keepdims=True
            )
            bias = jnp.where((kv_lane == r) & (hit > 0.0) & (kv_row < diag), 0.0, bias)
        for b in range(plan.kv_blocks):
            bias_rows[pl.ds(b * rows, rows), :] = jnp.broadcast_to(
                bias[b : b + 1, :], (rows, width)
            ).astype(jnp.bfloat16)

        exact = plan.chunk % 16 == 0
        for r in range(step):
            span = pl.ds(r * rows, rows)
            cols = pl.ds((head_from + r) * width, width)
            if far:
                piece = received[block // plan.per_group, :, :, cols]
                if not exact:
                    piece = piece.astype(jnp.float32)
                q_aug[span, pl.ds(0, width)] = piece.reshape(rows, width).astype(jnp.bfloat16)
            else:
                for c in range(n):
                    piece = (own if c == 0 else direct[c - 1])[
                        pl.ds(
                            pl.multiple_of(
                                plan.cache_rows(c)
                                + ((head_from + r) * slots + k) * plan.stride,
                                16,
                            ),
                            plan.chunk,
                        ),
                        :,
                    ]
                    if exact:
                        q_aug[
                            pl.ds(
                                pl.multiple_of(r * rows + (me ^ c) * plan.chunk, plan.chunk),
                                plan.chunk,
                            ),
                            pl.ds(0, width),
                        ] = piece
                    else:
                        loose[aligned(me ^ c, plan.chunk), :] = piece.astype(jnp.float32)
                if not exact:
                    q_aug[span, pl.ds(0, width)] = loose[...].astype(jnp.bfloat16)

        end = pl.multiple_of(diag * rows, rows)
        own_key = keys[pl.ds(end, rows), :]
        own_scale = scale[pl.ds(diag, 1), :]
        for r in range(step):
            span = pl.ds(r * rows, rows)
            s = lax.dot_general(
                q_aug[span, pl.ds(0, width)], own_key, NT, preferred_element_type=jnp.float32
            )
            s = jnp.where(causal, s * own_scale, MASKED)
            score[span, pl.ds(hold, width)] = s
            top[span, :] = s

        def find(size, first):
            def body(i, carry):
                start = first + i * size
                at = pl.multiple_of(start * rows, rows)
                span = pl.ds(at, size * rows)
                key = jnp.concatenate([keys[span, :], bias_rows[span, :]], axis=1)
                whole = lax.dot_general(q_aug[...], key, NT, preferred_element_type=jnp.float32)
                for r in range(step):
                    span = pl.ds(r * rows, rows)
                    best = top[span, :]
                    for m in range(size):
                        s = (
                            whole[r * rows : (r + 1) * rows, m * rows : (m + 1) * rows]
                            * scale[pl.ds(start + m, 1), :]
                        )
                        score[span, pl.ds(pl.multiple_of(at + m * rows, rows), width)] = s
                        best = jnp.maximum(best, s)
                    top[span, :] = best
                return carry

            return body

        def sweep(make):
            done = 0
            for size in SIZES:
                left = diag - done
                count = left // size if size > 2 else (left + 1) // 2
                lax.fori_loop(0, count, make(size, done), 0)
                done = done + count * size

        sweep(find)

        def summed(at, size):
            return jnp.concatenate(
                [values[pl.ds(at, size), :], jnp.ones((size, width), jnp.bfloat16)], axis=1
            )

        own_value = summed(end, rows)
        for r in range(step):
            span = pl.ds(r * rows, rows)
            m = jnp.broadcast_to(jnp.max(top[span, :], axis=1, keepdims=True), (rows, width))
            top[span, :] = m
            p = jnp.exp2(score[span, pl.ds(hold, width)] - m).astype(jnp.bfloat16)
            acc[span, :] = jnp.dot(p, own_value, preferred_element_type=jnp.float32)

        def gather(size, first):
            def body(i, carry):
                at = pl.multiple_of((first + i * size) * rows, rows)
                value = summed(at, size * rows)
                for r in range(step):
                    span = pl.ds(r * rows, rows)
                    m = jnp.concatenate([top[span, :]] * size, axis=1)
                    p = jnp.exp2(score[span, pl.ds(at, size * width)] - m).astype(jnp.bfloat16)
                    acc[span, :] += jnp.dot(p, value, preferred_element_type=jnp.float32)
                return carry

            return body

        sweep(gather)

        for r in range(step):
            cols = pl.ds((head_from + r) * width, width)
            if far:
                for c in range(n):
                    span = pl.ds(
                        pl.multiple_of(r * rows + (me ^ c) * plan.chunk, plan.chunk), plan.chunk
                    )
                    outs[c][k, :, cols] = (
                        acc[span, pl.ds(0, width)] / acc[span, pl.ds(width, width)]
                    ).astype(jnp.bfloat16)
            else:
                span = pl.ds(r * rows, rows)
                res = acc[span, pl.ds(0, width)] / acc[span, pl.ds(width, width)]
                if exact:
                    res = res.astype(jnp.bfloat16)
                out[target[block], :, :, cols] = res.reshape(n, plan.chunk, width).astype(
                    jnp.bfloat16
                )

    def slot(k, carry):
        for head_from in range(0, head_count, step):
            one(k, head_from)
        return carry

    lax.fori_loop(0, slots, slot, 0)


def attend(plan, far, target, operands):
    heads = plan.landed if far else plan.sourced
    step = heads
    while step > 1 and (
        heads % step or step * plan.rows * (plan.kv_rows + plan.width) * 4 > 18 * 2**20
    ):
        step -= 1
    n = plan.shards
    bf16, f32 = jnp.bfloat16, jnp.float32
    if far:
        shape = [
            jax.ShapeDtypeStruct((plan.slots, plan.chunk, heads * plan.width), bf16)
            for _ in range(n)
        ]
    else:
        table = jax.ShapeDtypeStruct((plan.kv_rows, plan.width), bf16)
        shape = [
            jax.ShapeDtypeStruct((plan.groups, n, plan.chunk, heads * plan.width), bf16),
            table,
            table,
            jax.ShapeDtypeStruct((plan.kv_blocks, plan.width), f32),
        ]
    work = plan.slots * heads * plan.rows * plan.kv_rows * plan.width
    held = (
        sum(x.size * x.dtype.itemsize for x in [*operands, *shape])
        + 2 * plan.kv_rows * plan.width
        + step * plan.rows * (plan.kv_rows + 6 * plan.width) * 4
    )
    return pl.pallas_call(
        functools.partial(attend_body, plan, far, step),
        in_specs=[SMEM] + [VMEM] * len(operands),
        out_specs=[VMEM] * len(shape),
        out_shape=shape,
        scratch_shapes=[
            pltpu.VMEM((step * plan.rows, 2 * plan.width), bf16),
            pltpu.VMEM((plan.kv_rows, plan.width), bf16),
            pltpu.VMEM((step * plan.rows, plan.kv_rows + plan.width), f32),
            pltpu.VMEM((step * plan.rows, plan.width), f32),
            pltpu.VMEM((step * plan.rows, 2 * plan.width), f32),
            pltpu.VMEM((plan.rows, plan.width), f32),
            pltpu.SMEM((plan.per_group,), jnp.int32),
        ],
        compiler_params=pltpu.CompilerParams(
            vmem_limit_bytes=min(held + 6 * 2**20, 62 * 2**20)
        ),
        cost_estimate=pl.CostEstimate(
            flops=2 * work, bytes_accessed=8 * 2**20, transcendentals=work // plan.width // 2
        ),
        name="attend_far" if far else "attend_near",
    )(target, *operands)


def place_rows(plan, target, received, *refs):
    parts, out, blocks = refs[: plan.shards], refs[plan.shards], refs[plan.shards + 1]
    group, me = lax.axis_index("replica"), lax.axis_index("ctx")

    def scan(j, found):
        hit = target[j] == group

        @pl.when(hit)
        def _():
            blocks[found] = j

        return found + hit.astype(jnp.int32)

    lax.fori_loop(0, target.shape[0], scan, 0)
    wide = plan.sourced * plan.width
    for k in range(plan.per_group):
        source = blocks[k] // plan.per_group
        part = blocks[k] % plan.per_group // plan.slots
        for h in range(plan.kv_heads):
            out[k, :, pl.ds(h * plan.span, wide)] = received[source, h * plan.repeat + part]
    for c in range(plan.shards):
        at = me ^ c
        head, part = at // plan.repeat, at % plan.repeat
        out[
            pl.ds(part * plan.slots, plan.slots),
            :,
            pl.ds(pl.multiple_of(head * plan.span + wide, plan.width), plan.landed * plan.width),
        ] = parts[c][...]


def per_device(queries, key_cache, value_cache, key_scale, value_scale, pattern, target):
    groups, shards = lax.axis_size("replica"), lax.axis_size("ctx")
    plan = Plan(queries, key_cache, key_scale, pattern, groups, shards)
    bf16 = jnp.bfloat16
    params = pltpu.CompilerParams(vmem_limit_bytes=32 * 2**20)

    def over_ctx(x, step):
        return lax.ppermute(x, "ctx", [(i, i ^ step) for i in range(shards)])

    def over_pair(x):
        return lax.ppermute(x, "replica", [(i, i ^ 1) for i in range(groups)])

    own, *pieces = pl.pallas_call(
        functools.partial(pack_near, plan),
        in_specs=[VMEM] * 5,
        out_specs=[VMEM] * shards,
        out_shape=[
            jax.ShapeDtypeStruct((plan.cache_rows(c) + plan.near_rows, plan.width), bf16)
            for c in range(shards)
        ],
        scratch_shapes=[pltpu.VMEM((plan.local_blocks, plan.width), jnp.float32)],
        compiler_params=params,
        name="pack_near",
    )(key_scale, value_scale, key_cache, value_cache, queries)
    direct = []
    for c, piece in enumerate(pieces):
        direct.append(over_ctx(piece, c + 1))
    swapped = [over_pair(piece) for piece in direct]
    far = pl.pallas_call(
        functools.partial(pack_far, plan),
        in_specs=[SMEM, VMEM],
        out_specs=VMEM,
        out_shape=jax.ShapeDtypeStruct(
            (groups, shards, plan.chunk, plan.landed * plan.width), bf16
        ),
        compiler_params=params,
        name="pack_far",
    )(target, queries)

    def everywhere(x):
        flat = x.reshape(groups * shards, *x.shape[2:])
        return lax.all_to_all(
            flat, ("replica", "ctx"), split_axis=0, concat_axis=0, tiled=True
        ).reshape(x.shape)

    rows_far = everywhere(far)
    done_near, keys, values, scale = attend(
        plan, False, target, [own, *direct, *swapped, pattern]
    )
    moved = everywhere(done_near)
    done_far = attend(plan, True, target, [rows_far, keys, values, scale, pattern])
    parts = [done_far[0]] + [over_ctx(done_far[c], c) for c in range(1, shards)]
    return pl.pallas_call(
        functools.partial(place_rows, plan),
        in_specs=[SMEM] + [VMEM] * (shards + 1),
        out_specs=VMEM,
        out_shape=jax.ShapeDtypeStruct(queries.shape, bf16),
        scratch_shapes=[pltpu.SMEM((plan.per_group,), jnp.int32)],
        compiler_params=params,
        name="place_rows",
    )(target, moved, *parts)


def solution(mesh):
    return jax.shard_map(
        per_device,
        mesh=mesh,
        in_specs=(
            P("replica", "ctx", None),
            P("ctx", None),
            P("ctx", None),
            P("ctx", None),
            P("ctx", None),
            P(),
            P(),
        ),
        out_specs=P("replica", "ctx", None),
        check_vma=False,
    )
```

```python
import functools
import math

import jax
import jax.numpy as jnp
from jax import lax
from jax.experimental import pallas as pl
from jax.experimental.pallas import tpu as pltpu
from jax.sharding import PartitionSpec as P


MASKED = -1e30
SIZES = (16, 8)
NT = (((1,), (1,)), ((), ()))
VMEM = pl.BlockSpec(memory_space=pltpu.VMEM)
SMEM = pl.BlockSpec(memory_space=pltpu.SMEM)
HBM = pl.BlockSpec(memory_space=pltpu.HBM)


class Plan:
    def __init__(self, queries, key_cache, key_scale, pattern, groups, shards):
        self.groups, self.shards = groups, shards
        self.per_group, self.chunk, self.row_width = queries.shape
        self.rows = self.chunk * shards
        self.kv_heads = key_scale.shape[1]
        self.width = key_cache.shape[1] // self.kv_heads
        self.group = self.row_width // self.width // self.kv_heads
        self.span = self.group * self.width
        self.local_blocks = key_scale.shape[0]
        self.local_rows = key_cache.shape[0]
        self.kv_blocks = self.local_blocks * shards
        self.kv_rows = self.local_rows * shards
        self.first_block = self.kv_blocks - pattern.shape[1]
        self.repeat = shards // self.kv_heads
        self.slots = self.per_group // self.repeat
        self.scale_rows = -(-3 * self.local_blocks // 16) * 16
        self.sourced = self.group * 3 // 7
        self.landed = self.group - self.sourced
        self.stride = max(self.chunk, 16)
        self.near_rows = self.sourced * self.slots * self.stride

    def cache_rows(self, relative):
        count = 2 * self.local_rows if relative == 0 else self.local_rows
        return count + self.scale_rows


def aligned(index, size):
    return pl.ds(pl.multiple_of(index * size, size), size)


def pack_far(plan, target, q_ref, far):
    group = lax.axis_index("replica")
    wide = plan.sourced * plan.width
    for d in range(plan.shards):
        head = d // plan.repeat
        for k in range(plan.per_group):
            far[target[group * plan.per_group + k], d] = q_ref[
                k, :, pl.ds(head * plan.span + wide, plan.landed * plan.width)
            ]


def pack_near(plan, ks_ref, vs_ref, k_ref, v_ref, q_ref, *refs):
    outs, factors = refs[: plan.shards], refs[plan.shards]
    group, me = lax.axis_index("replica"), lax.axis_index("ctx")
    rows, width, blocks = plan.rows, plan.width, plan.local_blocks
    half = group % 2
    head_row = lax.broadcasted_iota(jnp.int32, ks_ref.shape, 0)
    square = (blocks, blocks)
    own_block = lax.broadcasted_iota(jnp.int32, square, 0) == lax.broadcasted_iota(
        jnp.int32, square, 1
    )
    for c in range(plan.shards):
        at = me ^ c
        head, part = at // plan.repeat, at % plan.repeat
        lanes = aligned(head, width)

        def column(ref):
            line = jnp.sum(jnp.where(head_row == head, ref[...], 0.0), axis=0, keepdims=True)
            spread = jnp.where(own_block, jnp.broadcast_to(line, square), 0.0)
            return jnp.broadcast_to(jnp.sum(spread, axis=1, keepdims=True), (blocks, width))

        factors[...] = column(vs_ref)
        count = blocks if c == 0 else blocks // 2
        first = 0 if c == 0 else half * count
        out = outs[c]
        for i in range(count):
            b = first + i
            out[pl.ds(i * rows, rows), :] = k_ref[aligned(b, rows), lanes]
            out[pl.ds((count + i) * rows, rows), :] = (
                v_ref[aligned(b, rows), lanes].astype(jnp.float32) * factors[pl.ds(b, 1), :]
            ).astype(jnp.bfloat16)
        x = column(ks_ref)
        high = x.astype(jnp.bfloat16).astype(jnp.float32)
        middle = (x - high).astype(jnp.bfloat16).astype(jnp.float32)
        low = x - high - middle
        spare = plan.scale_rows - 3 * blocks
        terms = [high, middle, low]
        if spare:
            terms.append(jnp.zeros((spare, width), jnp.float32))
        out[pl.ds(2 * count * rows, plan.scale_rows), :] = jnp.concatenate(terms, axis=0).astype(
            jnp.bfloat16
        )
        base = plan.cache_rows(c)
        for r in range(plan.sourced):
            for k in range(plan.slots):
                out[pl.ds(base + (r * plan.slots + k) * plan.stride, plan.chunk), :] = q_ref[
                    part * plan.slots + k,
                    :,
                    pl.ds(pl.multiple_of(head * plan.span + r * width, width), width),
                ]


def attend_body(plan, far, step, *refs):
    n = plan.shards
    target, refs = refs[0], refs[1:]
    if far:
        received, key_in, value_in, scale, pattern = refs[:5]
        key_in_refs = [key_in, value_in]
        outs, refs = refs[5 : 5 + n], refs[5 + n :]
    else:
        own, direct, swapped = refs[0], refs[1:n], refs[n : 2 * n - 1]
        pattern, out, key_out, value_out, scale = refs[2 * n - 1 : 2 * n + 4]
        key_out_refs = [key_out, value_out]
        refs = refs[2 * n + 4 :]
    q_aug, bias_rows, score, top, acc, loose, blocks = refs[:7]
    moves = refs[7]
    if not far:
        key_out, value_out, keys, values = key_out_refs + list(refs[8:])
    else:
        key_in, value_in, keys, values = key_in_refs + list(refs[8:])

    group, me = lax.axis_index("replica"), lax.axis_index("ctx")
    rows, width, slots = plan.rows, plan.width, plan.slots
    head_count = plan.landed if far else plan.sourced
    head_first = plan.sourced if far else 0
    my_head, my_part = me // plan.repeat, me % plan.repeat
    half = group % 2

    def take(ref, count, block):
        size = count * rows
        at = pl.ds(pl.multiple_of(block * rows, rows), size)
        keys[at, :] = ref[pl.ds(0, size), :]
        values[at, :] = ref[pl.ds(size, size), :]

    if far:
        copies = [
            pltpu.make_async_copy(key_in, keys, moves.at[0]),
            pltpu.make_async_copy(value_in, values, moves.at[1]),
        ]
        for copy in copies:
            copy.start()
    else:
        size = plan.local_blocks
        some = size // 2
        factor = 1.0 / (math.sqrt(width) * math.log(2.0))
        for c in range(n):
            shard = me ^ c
            if c == 0:
                take(own, size, shard * size)
            else:
                take(direct[c - 1], some, shard * size + half * some)
                take(swapped[c - 1], some, shard * size + (1 - half) * some)
            tail = (own if c == 0 else direct[c - 1])[
                pl.ds(plan.cache_rows(c) - plan.scale_rows, plan.scale_rows), :
            ].astype(jnp.float32)
            scale[aligned(shard, size), :] = (
                tail[:size] + tail[size : 2 * size] + tail[2 * size : 3 * size]
            ) * factor
        copies = [
            pltpu.make_async_copy(keys, key_out, moves.at[0]),
            pltpu.make_async_copy(values, value_out, moves.at[1]),
        ]
        for copy in copies:
            copy.start()

    if far:

        def scan(j, found):
            hit = target[j] == group

            @pl.when(hit)
            def _():
                blocks[found] = j

            return found + hit.astype(jnp.int32)

        lax.fori_loop(0, target.shape[0], scan, 0)

    lane = lax.broadcasted_iota(jnp.int32, (rows, width), 1)
    causal = lane <= lax.broadcasted_iota(jnp.int32, (rows, width), 0)
    kv_lane = lax.broadcasted_iota(jnp.int32, (plan.kv_blocks, width), 1)
    selected = pattern.shape[2]
    kv_id = lax.broadcasted_iota(jnp.int32, (plan.kv_blocks, selected), 0)
    kv_row = lax.broadcasted_iota(jnp.int32, (plan.kv_blocks, width), 0)
    hold = score.shape[1] - width

    def block_of(k):
        if far:
            return blocks[my_part * slots + k]
        return group * plan.per_group + my_part * slots + k

    bias = jnp.full((plan.kv_blocks, width), MASKED, jnp.float32)
    for k in range(slots):
        block = block_of(k)
        for r in range(head_count):
            listed = pattern[my_head * plan.group + head_first + r, pl.ds(block, 1), :]
            hit = jnp.max(jnp.where(kv_id == listed, 1.0, 0.0), axis=1, keepdims=True)
            bias = jnp.where(
                (kv_lane == k * head_count + r)
                & (hit > 0.0)
                & (kv_row < plan.first_block + block),
                0.0,
                bias,
            )
    for b in range(plan.kv_blocks):
        bias_rows[pl.ds(b * rows, rows), :] = jnp.broadcast_to(
            bias[b : b + 1, :], (rows, width)
        ).astype(jnp.bfloat16)
    if far:
        for copy in copies:
            copy.wait()

    def one(k, head_from):
        block = block_of(k)
        diag = plan.first_block + block
        exact = plan.chunk % 16 == 0
        for r in range(step):
            span = pl.ds(r * rows, rows)
            cols = pl.ds((head_from + r) * width, width)
            tile = k * head_count + head_from + r
            q_aug[span, pl.ds(width, width)] = (lane == tile).astype(jnp.bfloat16)
            if far:
                piece = received[block // plan.per_group, :, :, cols]
                if not exact:
                    piece = piece.astype(jnp.float32)
                q_aug[span, pl.ds(0, width)] = piece.reshape(rows, width).astype(jnp.bfloat16)
            else:
                for c in range(n):
                    piece = (own if c == 0 else direct[c - 1])[
                        pl.ds(
                            pl.multiple_of(
                                plan.cache_rows(c)
                                + ((head_from + r) * slots + k) * plan.stride,
                                16,
                            ),
                            plan.chunk,
                        ),
                        :,
                    ]
                    if exact:
                        q_aug[
                            pl.ds(
                                pl.multiple_of(r * rows + (me ^ c) * plan.chunk, plan.chunk),
                                plan.chunk,
                            ),
                            pl.ds(0, width),
                        ] = piece
                    else:
                        loose[aligned(me ^ c, plan.chunk), :] = piece.astype(jnp.float32)
                if not exact:
                    q_aug[span, pl.ds(0, width)] = loose[...].astype(jnp.bfloat16)

        end = pl.multiple_of(diag * rows, rows)
        own_key = keys[pl.ds(end, rows), :]
        own_scale = scale[pl.ds(diag, 1), :]
        for r in range(step):
            span = pl.ds(r * rows, rows)
            s = lax.dot_general(
                q_aug[span, pl.ds(0, width)], own_key, NT, preferred_element_type=jnp.float32
            )
            s = jnp.where(causal, s * own_scale, MASKED)
            score[span, pl.ds(hold, width)] = s
            top[span, :] = s

        def find(size, first):
            def body(i, carry):
                start = first + i * size
                at = pl.multiple_of(start * rows, rows)
                span = pl.ds(at, size * rows)
                key = jnp.concatenate([keys[span, :], bias_rows[span, :]], axis=1)
                whole = lax.dot_general(q_aug[...], key, NT, preferred_element_type=jnp.float32)
                for r in range(step):
                    span = pl.ds(r * rows, rows)
                    best = top[span, :]
                    for m in range(size):
                        s = (
                            whole[r * rows : (r + 1) * rows, m * rows : (m + 1) * rows]
                            * scale[pl.ds(start + m, 1), :]
                        )
                        score[span, pl.ds(pl.multiple_of(at + m * rows, rows), width)] = s
                        best = jnp.maximum(best, s)
                    top[span, :] = best
                return carry

            return body

        big, small = SIZES
        left = diag % big
        wide = diag // big + (left > small).astype(jnp.int32)
        rest = ((left > 0) & (left <= small)).astype(jnp.int32)

        def sweep(make):
            lax.fori_loop(0, wide, make(big, 0), 0)
            lax.fori_loop(0, rest, make(small, wide * big), 0)

        sweep(find)

        def summed(at, size):
            return jnp.concatenate(
                [values[pl.ds(at, size), :], jnp.ones((size, width), jnp.bfloat16)], axis=1
            )

        own_value = summed(end, rows)
        for r in range(step):
            span = pl.ds(r * rows, rows)
            m = jnp.broadcast_to(jnp.max(top[span, :], axis=1, keepdims=True), (rows, width))
            top[span, :] = m
            p = jnp.exp2(score[span, pl.ds(hold, width)] - m).astype(jnp.bfloat16)
            acc[span, :] = jnp.dot(p, own_value, preferred_element_type=jnp.float32)

        def gather(size, first):
            def body(i, carry):
                at = pl.multiple_of((first + i * size) * rows, rows)
                value = summed(at, size * rows)
                for r in range(step):
                    span = pl.ds(r * rows, rows)
                    m = jnp.concatenate([top[span, :]] * size, axis=1)
                    p = jnp.exp2(score[span, pl.ds(at, size * width)] - m).astype(jnp.bfloat16)
                    acc[span, :] += jnp.dot(p, value, preferred_element_type=jnp.float32)
                return carry

            return body

        sweep(gather)

        for r in range(step):
            cols = pl.ds((head_from + r) * width, width)
            if far:
                for c in range(n):
                    span = pl.ds(
                        pl.multiple_of(r * rows + (me ^ c) * plan.chunk, plan.chunk), plan.chunk
                    )
                    outs[c][k, :, cols] = (
                        acc[span, pl.ds(0, width)] / acc[span, pl.ds(width, width)]
                    ).astype(jnp.bfloat16)
            else:
                span = pl.ds(r * rows, rows)
                res = acc[span, pl.ds(0, width)] / acc[span, pl.ds(width, width)]
                if exact:
                    res = res.astype(jnp.bfloat16)
                out[target[block], :, :, cols] = res.reshape(n, plan.chunk, width).astype(
                    jnp.bfloat16
                )

    def slot(k, carry):
        for head_from in range(0, head_count, step):
            one(k, head_from)
        return carry

    lax.fori_loop(0, slots, slot, 0)
    if not far:
        for copy in copies:
            copy.wait()


def attend(plan, far, target, operands):
    heads = plan.landed if far else plan.sourced
    step = heads
    while step > 1 and (
        heads % step or step * plan.rows * (plan.kv_rows + plan.width) * 4 > 18 * 2**20
    ):
        step -= 1
    n = plan.shards
    bf16, f32 = jnp.bfloat16, jnp.float32
    if far:
        shape = [
            jax.ShapeDtypeStruct((plan.slots, plan.chunk, heads * plan.width), bf16)
            for _ in range(n)
        ]
    else:
        table = jax.ShapeDtypeStruct((plan.kv_rows, plan.width), bf16)
        shape = [
            jax.ShapeDtypeStruct((plan.groups, n, plan.chunk, heads * plan.width), bf16),
            table,
            table,
            jax.ShapeDtypeStruct((plan.kv_blocks, plan.width), f32),
        ]
    work = plan.slots * heads * plan.rows * plan.kv_rows * plan.width
    held = (
        sum(x.size * x.dtype.itemsize for x in [*operands, *shape])
        + 2 * plan.kv_rows * plan.width
        + step * plan.rows * (plan.kv_rows + 6 * plan.width) * 4
    )
    return pl.pallas_call(
        functools.partial(attend_body, plan, far, step),
        in_specs=[SMEM]
        + ([VMEM, HBM, HBM, VMEM, VMEM] if far else [VMEM] * len(operands)),
        out_specs=[VMEM] * n if far else [VMEM, HBM, HBM, VMEM],
        out_shape=shape,
        scratch_shapes=[
            pltpu.VMEM((step * plan.rows, 2 * plan.width), bf16),
            pltpu.VMEM((plan.kv_rows, plan.width), bf16),
            pltpu.VMEM((step * plan.rows, plan.kv_rows + plan.width), f32),
            pltpu.VMEM((step * plan.rows, plan.width), f32),
            pltpu.VMEM((step * plan.rows, 2 * plan.width), f32),
            pltpu.VMEM((plan.rows, plan.width), f32),
            pltpu.SMEM((plan.per_group,), jnp.int32),
            pltpu.SemaphoreType.DMA((2,)),
            pltpu.VMEM((plan.kv_rows, plan.width), bf16),
            pltpu.VMEM((plan.kv_rows, plan.width), bf16),
        ],
        compiler_params=pltpu.CompilerParams(
            vmem_limit_bytes=min(held + 8 * 2**20, 62 * 2**20) if held > 28 * 2**20 else 52 * 2**20
        ),
        cost_estimate=pl.CostEstimate(
            flops=2 * work, bytes_accessed=8 * 2**20, transcendentals=work // plan.width // 2
        ),
        name="attend_far" if far else "attend_near",
    )(target, *operands)


def place_rows(plan, target, received, *refs):
    parts, out, blocks = refs[: plan.shards], refs[plan.shards], refs[plan.shards + 1]
    group, me = lax.axis_index("replica"), lax.axis_index("ctx")

    def scan(j, found):
        hit = target[j] == group

        @pl.when(hit)
        def _():
            blocks[found] = j

        return found + hit.astype(jnp.int32)

    lax.fori_loop(0, target.shape[0], scan, 0)
    wide = plan.sourced * plan.width
    for k in range(plan.per_group):
        source = blocks[k] // plan.per_group
        part = blocks[k] % plan.per_group // plan.slots
        for h in range(plan.kv_heads):
            out[k, :, pl.ds(h * plan.span, wide)] = received[source, h * plan.repeat + part]
    for c in range(plan.shards):
        at = me ^ c
        head, part = at // plan.repeat, at % plan.repeat
        out[
            pl.ds(part * plan.slots, plan.slots),
            :,
            pl.ds(pl.multiple_of(head * plan.span + wide, plan.width), plan.landed * plan.width),
        ] = parts[c][...]


def per_device(queries, key_cache, value_cache, key_scale, value_scale, pattern, target):
    groups, shards = lax.axis_size("replica"), lax.axis_size("ctx")
    plan = Plan(queries, key_cache, key_scale, pattern, groups, shards)
    bf16 = jnp.bfloat16
    params = pltpu.CompilerParams(vmem_limit_bytes=32 * 2**20)

    def over_ctx(x, step):
        return lax.ppermute(x, "ctx", [(i, i ^ step) for i in range(shards)])

    def over_pair(x):
        return lax.ppermute(x, "replica", [(i, i ^ 1) for i in range(groups)])

    own, *pieces = pl.pallas_call(
        functools.partial(pack_near, plan),
        in_specs=[VMEM] * 5,
        out_specs=[VMEM] * shards,
        out_shape=[
            jax.ShapeDtypeStruct((plan.cache_rows(c) + plan.near_rows, plan.width), bf16)
            for c in range(shards)
        ],
        scratch_shapes=[pltpu.VMEM((plan.local_blocks, plan.width), jnp.float32)],
        compiler_params=pltpu.CompilerParams(vmem_limit_bytes=60 * 2**20),
        name="pack_near",
    )(key_scale.T, value_scale.T, key_cache, value_cache, queries)
    direct = []
    for c, piece in enumerate(pieces):
        direct.append(over_ctx(piece, c + 1))
    swapped = []
    for piece in direct:
        swapped.append(over_pair(piece))
    far = pl.pallas_call(
        functools.partial(pack_far, plan),
        in_specs=[SMEM, VMEM],
        out_specs=VMEM,
        out_shape=jax.ShapeDtypeStruct(
            (groups, shards, plan.chunk, plan.landed * plan.width), bf16
        ),
        compiler_params=params,
        name="pack_far",
    )(target, queries)

    def everywhere(x):
        flat = x.reshape(groups * shards, *x.shape[2:])
        return lax.all_to_all(
            flat, ("replica", "ctx"), split_axis=0, concat_axis=0, tiled=True
        ).reshape(x.shape)

    rows_far = everywhere(far)
    done_near, keys, values, scale = attend(
        plan, False, target, [own, *direct, *swapped, pattern]
    )
    moved = everywhere(done_near)
    done_far = attend(plan, True, target, [rows_far, keys, values, scale, pattern])
    parts = [done_far[0]] + [over_ctx(done_far[c], c) for c in range(1, shards)]
    return pl.pallas_call(
        functools.partial(place_rows, plan),
        in_specs=[SMEM] + [VMEM] * (shards + 1),
        out_specs=VMEM,
        out_shape=jax.ShapeDtypeStruct(queries.shape, bf16),
        scratch_shapes=[pltpu.SMEM((plan.per_group,), jnp.int32)],
        compiler_params=params,
        name="place_rows",
    )(target, moved, *parts)


def solution(mesh):
    return jax.shard_map(
        per_device,
        mesh=mesh,
        in_specs=(
            P("replica", "ctx", None),
            P("ctx", None),
            P("ctx", None),
            P("ctx", None),
            P("ctx", None),
            P(),
            P(),
        ),
        out_specs=P("replica", "ctx", None),
        check_vma=False,
    )
```
